32 devices in a mesh: gx: 4 (over y, x), gy: 2 (over core), gz: 4 (over z).
Axes of the slice: x: 2, y: 2, z: 4, core: 2. Of those that a mesh axis runs over, the one named last changes fastest.
Arguments:
- initial: float32 [256, 64, 1024], P('gx', 'gy', 'gz'), may hold values from -6 to 6
- right_side: float32 [256, 64, 1024], P('gx', 'gy', 'gz'), may hold values from -12 to 12
- shift_field: float32 [256, 64, 1024], P('gx', 'gy', 'gz'), may hold values from 0.5 to 8
Outputs:
- relaxed: float32 [256, 64, 1024], P('gx', 'gy', 'gz')
The draws below stay inside these ranges and needn't reach their ends.
All inputs are finite; a program needn't handle non-finite values.
Results may differ from the reference program's by a relative error of at most 0.00002.
Values sent between devices are 32-bit elements; how exact they have to be, the bound alone decides.
A program may use at most 128 MiB of HBM per device.

```python
import math
import jax
import jax.numpy as jnp

SWEEPS = 4
NX = 256
NY = 64
NZ = 1024


def levels(stream_key, extent, cuts, least, high):
    def one(position, parts):
        heights = jax.random.uniform(jax.random.fold_in(jax.random.fold_in(stream_key, 6), position), (parts,), jnp.float32, least / len(cuts), high / len(cuts))
        return jnp.repeat(jnp.exp(heights), extent[position] // parts).reshape((-1,) + (1,) * (len(extent) - position - 1))

    gain = one(*cuts[0])
    for cut in cuts[1:]:
        gain = gain * one(*cut)
    return gain


def centred(stream_key, extent, scale, limit, pieces=(), held_as=jnp.bfloat16):
    array = scale * jax.random.normal(stream_key, extent, jnp.float32)
    if pieces:
        array = array * levels(stream_key, extent, pieces, -0.22, 0.18)
    return jnp.clip(array, -limit, limit).astype(held_as)


def setup_inputs(seed: int = 0) -> dict:
    keys = jax.random.split(jax.random.key(seed), 4)
    initial = centred(keys[0], (NX, NY, NZ), 1.0, 6.0, ((0, 4), (1, 2), (2, 4)), jnp.float32)
    right_side = centred(keys[1], (NX, NY, NZ), 2.0, 12.0, ((0, 4), (1, 2), (2, 4)), jnp.float32)
    shift_field = jnp.clip(jnp.exp(math.log(8.0) - 2.7725887 * jax.random.uniform(keys[2], (NX, NY, NZ), jnp.float32) ** levels(keys[2], (NX, NY, NZ), ((0, 4), (1, 2), (2, 4)), -0.2, 0.2)), 0.5, 8.0)
    return dict(initial=initial, right_side=right_side, shift_field=shift_field)


relax_weight = 0.8


def neighbours(field):
    total = jnp.roll(field, 1, 0) + jnp.roll(field, -1, 0)
    total = total + jnp.roll(field, 1, 1) + jnp.roll(field, -1, 1)
    total = total + jnp.roll(field, 1, 2) + jnp.roll(field, -1, 2)
    return total


def reference(initial, right_side, shift_field):
    diagonal = 6.0 + shift_field
    relaxed = initial
    for sweep in range(SWEEPS):
        beside = neighbours(relaxed)
        relaxed = relaxed + relax_weight * (right_side - (diagonal * relaxed - beside)) / diagonal
    return relaxed
```

```python
import functools

import jax
import jax.numpy as jnp
import numpy as np
from jax import lax
from jax.experimental import pallas as pl
from jax.experimental.pallas import tpu as pltpu
from jax.sharding import PartitionSpec as P

SWEEPS = 4
WEIGHT = np.float32(0.8)
KEEP = np.float32(1.0) - WEIGHT
AXES = ("gx", "gy", "gz")
MESH = pl.DeviceIdType.MESH
ROWS = 8
LANES = 128


def beside(axis, step):
    count = lax.axis_size(axis)
    return {axis: lax.rem(lax.axis_index(axis) + (count + step), count)}


def iota(dim, shape):
    return lax.broadcasted_iota(jnp.int32, shape, dim)


def turned(block, shift, dim):
    size = block.shape[dim]
    shift = shift % size
    return block if shift == 0 else pltpu.roll(block, shift, dim)


def kernel(init_ref, rhs_ref, shift_ref, out_ref, v, q, w, ys, yh, zs, zh, load, send, recv):
    nx, ny, nz = out_ref.shape
    groups, bands, tiles = nx // ROWS, ny // ROWS, nz // LANES

    barrier = pltpu.get_barrier_semaphore()
    for axis in AXES:
        for step in (-1, 1):
            pl.semaphore_signal(barrier, inc=1, device_id=beside(axis, step), device_id_type=MESH)

    def init_copy(g):
        return pltpu.make_async_copy(
            init_ref.at[pl.ds(g * ROWS, ROWS)], v.at[0, pl.ds(g * ROWS + 1, ROWS)], load.at[g]
        )

    for g in range(groups):
        init_copy(g).start()
    rhs_copy = pltpu.make_async_copy(rhs_ref, q, load.at[groups])
    shift_copy = pltpu.make_async_copy(shift_ref, w, load.at[groups + 1])
    rhs_copy.start()
    shift_copy.start()

    def remote(src, dst, t, face, axis, step):
        return pltpu.make_async_remote_copy(
            src_ref=src,
            dst_ref=dst,
            send_sem=send.at[t, face],
            recv_sem=recv.at[t, face],
            device_id=beside(axis, step),
            device_id_type=MESH,
        )

    def x_copies(t):
        low = init_ref.at[0] if t == 0 else v.at[t, 1]
        high = init_ref.at[nx - 1] if t == 0 else v.at[t, nx]
        return (
            remote(high, v.at[t, 0], t, 0, "gx", 1),
            remote(low, v.at[t, nx + 1], t, 1, "gx", -1),
        )

    def z_copies(t):
        return (
            remote(zs.at[t, 1], zh.at[t, 0], t, 4, "gz", 1),
            remote(zs.at[t, 0], zh.at[t, 1], t, 5, "gz", -1),
        )

    def y_copies(t):
        return (
            remote(ys.at[t, 1], yh.at[t, 0], t, 2, "gy", 1),
            remote(ys.at[t, 0], yh.at[t, 1], t, 3, "gy", -1),
        )

    row = iota(0, (ROWS, nz))
    lane = iota(1, (ny, LANES))

    def pack(t, g, planes, carry):
        y_low, y_high = jnp.zeros((2, ROWS, nz), jnp.float32)
        z_low, z_high = jnp.zeros((2, ny, LANES), jnp.float32)
        for j, new in enumerate(planes):
            y_low = jnp.where(row == j, turned(new[:ROWS], j, 0), y_low)
            y_high = jnp.where(row == j, turned(new[ny - ROWS :], j + 1, 0), y_high)
            z_low = jnp.where(lane == j, turned(new[:, :LANES], j, 1), z_low)
            z_high = jnp.where(lane == j, turned(new[:, nz - LANES :], j + 1, 1), z_high)
        ys[t, 0, pl.ds(pl.multiple_of(g * ROWS, ROWS), ROWS)] = y_low
        ys[t, 1, pl.ds(pl.multiple_of(g * ROWS, ROWS), ROWS)] = y_high
        place = g * ROWS
        return (
            carry[0] + pltpu.roll(z_low, place, 1),
            carry[1] + pltpu.roll(z_high, place, 1),
        )

    def send_packed(t, carry):
        zs[t, 0] = carry[0]
        zs[t, 1] = carry[1]
        for copy in z_copies(t) + y_copies(t):
            copy.start()

    blank = (jnp.zeros((ny, LANES), jnp.float32), jnp.zeros((ny, LANES), jnp.float32))

    pl.semaphore_wait(barrier, 2 * len(AXES))
    for copy in x_copies(0):
        copy.start()

    def first_pack(g, carry):
        init_copy(g).wait()
        planes = [v[0, g * ROWS + 1 + j] for j in range(ROWS)]
        return pack(0, g, planes, carry)

    send_packed(0, lax.fori_loop(0, groups, first_pack, blank))

    rhs_copy.wait()
    shift_copy.wait()

    def prepare(x, carry):
        ratio = WEIGHT / (6.0 + w[x])
        w[x] = ratio
        q[x] = ratio * q[x]
        return carry

    lax.fori_loop(0, nx, prepare, 0)

    def relax_group(t, g, carry):
        base = g * ROWS
        aligned = pl.multiple_of(base, ROWS)
        y_low = yh[t, 0, pl.ds(aligned, ROWS)]
        y_high = yh[t, 1, pl.ds(aligned, ROWS)]
        back = lax.rem(LANES - base, LANES)
        z_low = pltpu.roll(zh[t, 0], back, 1)
        z_high = pltpu.roll(zh[t, 1], back, 1)
        planes = []
        for j in range(ROWS):
            c = v[t, base + 1 + j]
            total = v[t, base + j] + v[t, base + 2 + j]
            before = [turned(c[ROWS * k : ROWS * k + ROWS], 1, 0) for k in range(bands)]
            after = [turned(c[ROWS * k : ROWS * k + ROWS], -1, 0) for k in range(bands)]
            before_edge = [turned(y_low, -j, 0)] + before[:-1]
            after_edge = after[1:] + [turned(y_high, ROWS - 1 - j, 0)]
            total = total + jnp.concatenate(
                [
                    jnp.where(row == 0, before_edge[k], before[k])
                    + jnp.where(row == ROWS - 1, after_edge[k], after[k])
                    for k in range(bands)
                ],
                axis=0,
            )
            before = [turned(c[:, LANES * k : LANES * k + LANES], 1, 1) for k in range(tiles)]
            after = [turned(c[:, LANES * k : LANES * k + LANES], -1, 1) for k in range(tiles)]
            before_edge = [turned(z_low, -j, 1)] + before[:-1]
            after_edge = after[1:] + [turned(z_high, LANES - 1 - j, 1)]
            total = total + jnp.concatenate(
                [
                    jnp.where(lane == 0, before_edge[k], before[k])
                    + jnp.where(lane == LANES - 1, after_edge[k], after[k])
                    for k in range(tiles)
                ],
                axis=1,
            )
            new = (KEEP * c + q[base + j]) + w[base + j] * total
            if t + 1 < SWEEPS:
                v[t + 1, base + 1 + j] = new
                planes.append(new)
            else:
                out_ref[base + j] = new
        if t + 1 < SWEEPS:
            carry = pack(t + 1, g, planes, carry)
        return carry

    for t in range(SWEEPS):
        for copy in x_copies(t) + y_copies(t) + z_copies(t):
            copy.wait()
        body = functools.partial(relax_group, t)
        if t + 1 < SWEEPS:
            carry = lax.fori_loop(0, 2, lambda i, c: body(i * (groups - 1), c), blank)
            for copy in x_copies(t + 1):
                copy.start()
            send_packed(t + 1, lax.fori_loop(1, groups - 1, body, carry))
        else:
            lax.fori_loop(0, groups, body, 0)


def shards(initial, right_side, shift_field):
    nx, ny, nz = initial.shape
    assert nx % ROWS == 0 and 2 * ROWS <= nx <= LANES
    assert ny % ROWS == 0 and nz % LANES == 0
    faces = 2 * len(AXES)
    return pl.pallas_call(
        kernel,
        out_shape=pltpu.VMEM((nx, ny, nz), jnp.float32),
        in_specs=[pl.BlockSpec(memory_space=pltpu.HBM)] * 3,
        out_specs=pl.BlockSpec(memory_space=pltpu.VMEM),
        scratch_shapes=[
            pltpu.VMEM((SWEEPS, nx + 2, ny, nz), jnp.float32),
            pltpu.VMEM((nx, ny, nz), jnp.float32),
            pltpu.VMEM((nx, ny, nz), jnp.float32),
            pltpu.VMEM((SWEEPS, 2, nx, nz), jnp.float32),
            pltpu.VMEM((SWEEPS, 2, nx, nz), jnp.float32),
            pltpu.VMEM((SWEEPS, 2, ny, LANES), jnp.float32),
            pltpu.VMEM((SWEEPS, 2, ny, LANES), jnp.float32),
            pltpu.SemaphoreType.DMA((nx // ROWS + 2,)),
            pltpu.SemaphoreType.DMA((SWEEPS, faces)),
            pltpu.SemaphoreType.DMA((SWEEPS, faces)),
        ],
        compiler_params=pltpu.CompilerParams(
            collective_id=0, has_side_effects=True, vmem_limit_bytes=32 * 1024 * 1024
        ),
    )(*(pltpu.with_memory_space_constraint(a, pltpu.HBM) for a in (initial, right_side, shift_field)))


def solution(mesh):
    spec = P(*AXES)
    return jax.shard_map(
        shards, mesh=mesh, in_specs=(spec, spec, spec), out_specs=spec, check_vma=False
    )
```

```python
import functools

import jax
import jax.numpy as jnp
import numpy as np
from jax import lax
from jax.experimental import pallas as pl
from jax.experimental.pallas import tpu as pltpu
from jax.sharding import PartitionSpec as P

SWEEPS = 4
WEIGHT = np.float32(0.8)
KEEP = np.float32(1.0) - WEIGHT
AXES = ("gx", "gy", "gz")
MESH = pl.DeviceIdType.MESH
ROWS = 8
LANES = 128


def beside(axis, step):
    count = lax.axis_size(axis)
    return {axis: lax.rem(lax.axis_index(axis) + (count + step), count)}


def iota(dim, shape):
    return lax.broadcasted_iota(jnp.int32, shape, dim)


def turned(block, shift, dim):
    size = block.shape[dim]
    shift = shift % size
    return block if shift == 0 else pltpu.roll(block, shift, dim)


def kernel(init_ref, rhs_ref, shift_ref, out_ref, v, q, w, ys, yh, zs, zh, zp, wz, load, send, recv):
    nx, ny, nz = out_ref.shape
    groups, bands, tiles = nx // ROWS, ny // ROWS, nz // LANES

    barrier = pltpu.get_barrier_semaphore()
    for axis in AXES:
        for step in (-1, 1):
            pl.semaphore_signal(barrier, inc=1, device_id=beside(axis, step), device_id_type=MESH)

    def init_copy(g):
        return pltpu.make_async_copy(
            init_ref.at[pl.ds(g * ROWS, ROWS)], v.at[0, pl.ds(g * ROWS + 1, ROWS)], load.at[g]
        )

    for g in range(groups):
        init_copy(g).start()
    rhs_copy = pltpu.make_async_copy(rhs_ref, q, load.at[groups])
    shift_copy = pltpu.make_async_copy(shift_ref, w, load.at[groups + 1])
    rhs_copy.start()
    shift_copy.start()

    def remote(src, dst, t, face, axis, step):
        return pltpu.make_async_remote_copy(
            src_ref=src,
            dst_ref=dst,
            send_sem=send.at[t, face],
            recv_sem=recv.at[t, face],
            device_id=beside(axis, step),
            device_id_type=MESH,
        )

    def x_copies(t):
        low = init_ref.at[0] if t == 0 else v.at[t, 1]
        high = init_ref.at[nx - 1] if t == 0 else v.at[t, nx]
        return (
            remote(high, v.at[t, 0], t, 0, "gx", 1),
            remote(low, v.at[t, nx + 1], t, 1, "gx", -1),
        )

    def z_copies(t):
        return (
            remote(zs.at[t, 1], zh.at[t, 0], t, 4, "gz", 1),
            remote(zs.at[t, 0], zh.at[t, 1], t, 5, "gz", -1),
        )

    def y_copies(t):
        return (
            remote(ys.at[t, 1], yh.at[t, 0], t, 2, "gy", 1),
            remote(ys.at[t, 0], yh.at[t, 1], t, 3, "gy", -1),
        )

    row = iota(0, (ROWS, nz))
    row1 = iota(0, (ROWS, LANES))
    lane = iota(1, (ny, LANES))
    lane1 = iota(1, (ROWS, LANES))

    def put(t, x, new):
        if t < SWEEPS:
            v[t, x + 1] = new
        else:
            out_ref[x] = new

    def get(t, x):
        return v[t, x + 1] if t < SWEEPS else out_ref[x]

    def pack_rows(t, g, planes):
        low, high = jnp.zeros((2, ROWS, nz), jnp.float32)
        for j, new in enumerate(planes):
            low = jnp.where(row == j, turned(new[:ROWS], j, 0), low)
            high = jnp.where(row == j, turned(new[ny - ROWS :], j + 1, 0), high)
        ys[t, 0, pl.ds(pl.multiple_of(g * ROWS, ROWS), ROWS)] = low
        ys[t, 1, pl.ds(pl.multiple_of(g * ROWS, ROWS), ROWS)] = high

    def pack_columns(g, planes, carry):
        low, high = jnp.zeros((2, ny, LANES), jnp.float32)
        for j, new in enumerate(planes):
            low = jnp.where(lane == j, turned(new[:, :LANES], j, 1), low)
            high = jnp.where(lane == j, turned(new[:, nz - LANES :], j + 1, 1), high)
        return carry[0] + pltpu.roll(low, g * ROWS, 1), carry[1] + pltpu.roll(high, g * ROWS, 1)

    def start(copies):
        for copy in copies:
            copy.start()

    def wait(copies):
        for copy in copies:
            copy.wait()

    blank = (jnp.zeros((ny, LANES), jnp.float32), jnp.zeros((ny, LANES), jnp.float32))

    pl.semaphore_wait(barrier, 2 * len(AXES))
    start(x_copies(0))

    def first_pack(g, carry):
        init_copy(g).wait()
        planes = [v[0, g * ROWS + 1 + j] for j in range(ROWS)]
        pack_rows(0, g, planes)
        return pack_columns(g, planes, carry)

    packed = lax.fori_loop(0, groups, first_pack, blank)
    zs[0, 0], zs[0, 1] = packed
    start(z_copies(0) + y_copies(0))

    rhs_copy.wait()
    shift_copy.wait()

    def prepare(g, carry):
        planes = []
        for j in range(ROWS):
            x = g * ROWS + j
            ratio = WEIGHT / (6.0 + w[x])
            w[x] = ratio
            q[x] = ratio * q[x]
            planes.append(ratio)
        return pack_columns(g, planes, carry)

    packed = lax.fori_loop(0, groups, prepare, blank)
    wz[0], wz[1] = packed

    def blend(t, x, k, y_low, y_high, z_low, z_high):
        at = slice(ROWS * k, ROWS * k + ROWS)
        c = v[t, x + 1, at]
        total = v[t, x, at] + v[t, x + 2, at]
        above = v[t, x + 1, ROWS * k - ROWS : ROWS * k] if k else None
        below = v[t, x + 1, ROWS * k + ROWS : ROWS * k + 2 * ROWS] if k + 1 < bands else None
        above = turned(above, 1, 0) if k else y_low
        below = turned(below, -1, 0) if k + 1 < bands else y_high
        total = total + jnp.where(row == 0, above, turned(c, 1, 0))
        total = total + jnp.where(row == ROWS - 1, below, turned(c, -1, 0))
        before = [turned(c[:, LANES * i : LANES * i + LANES], 1, 1) for i in range(tiles)]
        after = [turned(c[:, LANES * i : LANES * i + LANES], -1, 1) for i in range(tiles)]
        before_edge = [z_low] + before[:-1]
        after_edge = after[1:] + [z_high]
        total = total + jnp.concatenate(
            [
                jnp.where(lane1 == 0, before_edge[i], before[i])
                + jnp.where(lane1 == LANES - 1, after_edge[i], after[i])
                for i in range(tiles)
            ],
            axis=1,
        )
        return (KEEP * c + q[x, at]) + w[x, at] * total

    def bulk_group(t, ks, g, carry, first=0, last=ROWS):
        base = g * ROWS
        aligned = pl.multiple_of(base, ROWS)
        y_low = yh[t, 0, pl.ds(aligned, ROWS)] if 0 in ks else None
        y_high = yh[t, 1, pl.ds(aligned, ROWS)] if bands - 1 in ks else None
        none = jnp.zeros((ROWS, LANES), jnp.float32)
        low = [none for _ in ks]
        high = [none for _ in ks]
        for j in range(first, last):
            x = base + j
            for i, k in enumerate(ks):
                new = blend(
                    t,
                    x,
                    k,
                    turned(y_low, -j, 0) if k == 0 else None,
                    turned(y_high, ROWS - 1 - j, 0) if k == bands - 1 else None,
                    none,
                    none,
                )
                if t + 1 < SWEEPS:
                    v[t + 1, x + 1, ROWS * k : ROWS * k + ROWS] = new
                else:
                    out_ref[x, ROWS * k : ROWS * k + ROWS] = new
                low[i] = jnp.where(lane1 == j, turned(new[:, :LANES], j, 1), low[i])
                high[i] = jnp.where(lane1 == j, turned(new[:, nz - LANES :], j + 1, 1), high[i])
        return tuple(
            old + pltpu.roll(add, base, 1) for old, add in zip(carry, low + high)
        )

    def bulk(t, ks):
        none = jnp.zeros((ROWS, LANES), jnp.float32)
        carry = bulk_group(t, ks, 0, (none,) * (2 * len(ks)), first=1)
        carry = lax.fori_loop(1, groups - 1, functools.partial(bulk_group, t, ks), carry)
        carry = bulk_group(t, ks, groups - 1, carry, last=ROWS - 1)
        for i, k in enumerate(ks):
            zp[0, ROWS * k : ROWS * k + ROWS] = carry[i]
            zp[1, ROWS * k : ROWS * k + ROWS] = carry[len(ks) + i]

    def edge_plane(t, x):
        base = x // ROWS * ROWS
        j = x - base
        parts = []
        for k in range(bands):
            at = slice(ROWS * k, ROWS * k + ROWS)
            parts.append(
                blend(
                    t,
                    x,
                    k,
                    turned(yh[t, 0, base : base + ROWS], -j, 0),
                    turned(yh[t, 1, base : base + ROWS], ROWS - 1 - j, 0),
                    turned(zh[t, 0, at], -x, 1),
                    turned(zh[t, 1, at], LANES - 1 - x, 1),
                )
            )
        return jnp.concatenate(parts, axis=0)

    def mend_group(t, g, carry, first=0, last=ROWS):
        base = g * ROWS
        back = lax.rem(LANES - base, LANES)
        z_low = pltpu.roll(zs[t, 0], back, 1)
        z_high = pltpu.roll(zs[t, 1], back, 1)
        planes = []
        for j in range(ROWS):
            plane = get(t, base + j)
            if first <= j < last:
                parts = [plane[:, LANES * i : LANES * i + LANES] for i in range(tiles)]
                parts[0] = jnp.where(lane == 0, turned(z_low, -j, 1), parts[0])
                parts[-1] = jnp.where(lane == LANES - 1, turned(z_high, LANES - 1 - j, 1), parts[-1])
                plane = jnp.concatenate(parts, axis=1)
                put(t, base + j, plane)
            planes.append(plane)
        if t < SWEEPS:
            pack_rows(t, g, planes)
        return carry

    outer = tuple(sorted({0, bands - 1}))
    inner = tuple(range(1, bands - 1))
    for t in range(SWEEPS):
        if inner:
            bulk(t, inner)
        wait(y_copies(t))
        bulk(t, outer)
        wait(x_copies(t) + z_copies(t))
        first_plane, last_plane = edge_plane(t, 0), edge_plane(t, nx - 1)
        put(t + 1, 0, first_plane)
        put(t + 1, nx - 1, last_plane)
        if t + 1 < SWEEPS:
            start(x_copies(t + 1))
        for side, cut, turn in ((0, slice(0, LANES), 0), (1, slice(nz - LANES, nz), 1)):
            face = zp[side] + wz[side] * zh[t, side]
            face = jnp.where(lane == 0, turned(first_plane[:, cut], turn, 1), face)
            face = jnp.where(lane == nx - 1, turned(last_plane[:, cut], nx - 1 + turn, 1), face)
            zs[t + 1, side] = face
        if t + 1 < SWEEPS:
            start(z_copies(t + 1))
        mend_group(t + 1, 0, 0, first=1)
        lax.fori_loop(1, groups - 1, functools.partial(mend_group, t + 1), 0)
        mend_group(t + 1, groups - 1, 0, last=ROWS - 1)
        if t + 1 < SWEEPS:
            start(y_copies(t + 1))


def shards(initial, right_side, shift_field):
    nx, ny, nz = initial.shape
    assert nx % ROWS == 0 and 2 * ROWS <= nx <= LANES
    assert ny % ROWS == 0 and nz % LANES == 0
    faces = 2 * len(AXES)
    return pl.pallas_call(
        kernel,
        out_shape=pltpu.VMEM((nx, ny, nz), jnp.float32),
        in_specs=[pl.BlockSpec(memory_space=pltpu.HBM)] * 3,
        out_specs=pl.BlockSpec(memory_space=pltpu.VMEM),
        scratch_shapes=[
            pltpu.VMEM((SWEEPS, nx + 2, ny, nz), jnp.float32),
            pltpu.VMEM((nx, ny, nz), jnp.float32),
            pltpu.VMEM((nx, ny, nz), jnp.float32),
            pltpu.VMEM((SWEEPS, 2, nx, nz), jnp.float32),
            pltpu.VMEM((SWEEPS, 2, nx, nz), jnp.float32),
            pltpu.VMEM((SWEEPS + 1, 2, ny, LANES), jnp.float32),
            pltpu.VMEM((SWEEPS, 2, ny, LANES), jnp.float32),
            pltpu.VMEM((2, ny, LANES), jnp.float32),
            pltpu.VMEM((2, ny, LANES), jnp.float32),
            pltpu.SemaphoreType.DMA((nx // ROWS + 2,)),
            pltpu.SemaphoreType.DMA((SWEEPS, faces)),
            pltpu.SemaphoreType.DMA((SWEEPS, faces)),
        ],
        compiler_params=pltpu.CompilerParams(
            collective_id=0, has_side_effects=True, vmem_limit_bytes=32 * 1024 * 1024
        ),
    )(*(pltpu.with_memory_space_constraint(a, pltpu.HBM) for a in (initial, right_side, shift_field)))


def solution(mesh):
    spec = P(*AXES)
    return jax.shard_map(
        shards, mesh=mesh, in_specs=(spec, spec, spec), out_specs=spec, check_vma=False
    )
```
